32 devices in a mesh: facet: 4 (over y, core), team: 4 (over z), sub: 2 (over x).
Axes of the slice: x: 2, y: 2, z: 4, core: 2. Of those that a mesh axis runs over, the one named last changes fastest.
Arguments:
- facet_rows: bfloat16 [4, 2, 32, 4096], P('facet', None, 'team'), may hold values from -6 to 6
- sub_offsets: int32 [8, 2], replicated, may hold values from 0 to 4095
- facet_offsets: int32 [4, 2], replicated, may hold values from 0 to 4095
- aterm: bfloat16 [4, 2, 256, 256], P('facet'), may hold values from 0.29882812 to 3
- cells: int32 [4, 2, 4, 2, 256], P('facet', None, 'team'), may hold values from 0 to 1023
- observed: bfloat16 [4, 2, 4, 2, 256], P('facet', None, 'team'), may hold values from -6 to 6
- weights: bfloat16 [4, 2, 4, 256], P('facet', None, 'team'), may hold values from 0.29882812 to 3
- counts: int32 [4, 2, 4], replicated, may hold values from 1 to 256, as said below
Outputs:
- facet_update: float32 [4, 2, 32, 4096], P('facet', None, 'team', 'sub')
The draws below stay inside these ranges and needn't reach their ends.
Inputs may be any that keep to these rules, and one draw needn't show every extreme that they name: Slots 0 to counts[a, b, t] - 1 are live. For every a and t one of the two subgrids with indices [a, 0] and [a, 1] has at most 64 live slots, and which of the two it is does not change with t.
All inputs are finite; a program needn't handle non-finite values.
Results may differ from the reference program's by a relative error of at most 0.019.
Values may be sent and summed in bfloat16 or wider, within the bound.
A program may use at most 64 MiB of HBM per device.

```python
import math
import jax
import jax.numpy as jnp
from jax import lax

L = 4096
M = 128
SG = 256
VDEV = 256
R = 32
NS = 8
N_FACET = 4
N_TEAM = 4
N_SUB = 2


def draw_counts(key, part):
    key_list = jax.random.split(jax.random.fold_in(key, 7), 5)
    heavy_side = jax.random.randint(key_list[0], (N_FACET, 1), 0, 2)
    heavy_loads = jax.random.randint(key_list[1], (N_FACET, N_TEAM), VDEV // 2, VDEV + 1)
    light_loads = jax.random.randint(key_list[2], (N_FACET, N_TEAM), 1, VDEV // 4 + 1)
    flat_ids = jnp.arange(N_FACET * N_TEAM, dtype=jnp.int32).reshape(N_FACET, N_TEAM)
    top_pick = jax.random.randint(key_list[3], (), 0, N_FACET * N_TEAM)
    low_pick = jax.random.randint(key_list[4], (), 0, N_FACET * N_TEAM)
    heavy_loads = jnp.where(flat_ids == top_pick, VDEV, heavy_loads)
    light_loads = jnp.where(flat_ids == low_pick, VDEV // 4, light_loads)
    side_zero = jnp.where(heavy_side == 0, heavy_loads, light_loads)
    side_one = jnp.where(heavy_side == 0, light_loads, heavy_loads)
    return jnp.stack([side_zero, side_one], 1).astype(jnp.int32)


def place_ends(entries, rng, least, top_value):
    longest = entries.shape.index(max(entries.shape))
    spots = []
    for shift in (0, 1):
        where = [jax.random.randint(jax.random.fold_in(rng, axis), (), 0, length) for axis, length in enumerate(entries.shape)]
        where[longest] = (where[longest] + shift) % entries.shape[longest]
        spots.append(tuple(where))
    return entries.at[spots[0]].set(least).at[spots[1]].set(top_value)


def block_scale(stream_key, extent, cuts, least, largest):
    level = 1.0
    for axis_at, shards_of in cuts:
        heights = jax.random.uniform(jax.random.fold_in(jax.random.fold_in(stream_key, 6), axis_at), (shards_of,), jnp.float32, least / len(cuts), largest / len(cuts))
        level = level * jnp.repeat(jnp.exp(heights), extent[axis_at] // shards_of).reshape((-1,) + (1,) * (len(extent) - 1 - axis_at))
    return level


def noise(stream_key, extent, scale, most, cuts=(), kind=jnp.bfloat16):
    entries = scale * jax.random.normal(stream_key, extent, jnp.float32)
    if cuts:
        entries = entries * block_scale(stream_key, extent, cuts, -0.22, 0.18)
    return jnp.clip(entries, -most, most).astype(kind)


def setup_inputs(seed: int = 0) -> dict:
    splits = jax.random.split(jax.random.key(seed), 9)
    return {
        "facet_rows": noise(splits[0], (N_FACET, 2, R, L), 1.0, 6.0, ((0, 4), (2, 4))),
        "sub_offsets": place_ends(jax.random.randint(splits[1], (NS, 2), 0, L), jax.random.fold_in(splits[1], 1), 0, L - 1).astype(jnp.int32),
        "facet_offsets": place_ends(jax.random.randint(splits[2], (N_FACET, 2), 0, L), jax.random.fold_in(splits[2], 1), 0, L - 1).astype(jnp.int32),
        "aterm": jnp.clip(jnp.exp(math.log(3.0) - 2.306499 * jax.random.uniform(splits[3], (N_FACET, N_SUB, SG, SG), jnp.float32) ** block_scale(splits[3], (N_FACET, N_SUB, SG, SG), ((0, 4),), -0.2, 0.2)), 0.29882812, 3.0).astype(jnp.bfloat16),
        "cells": place_ends(jax.random.randint(splits[4], (N_FACET, N_SUB, N_TEAM, 2, VDEV), 0, 4 * SG), jax.random.fold_in(splits[4], 1), 0, (4 * SG) - 1).astype(jnp.int32),
        "observed": noise(splits[5], (N_FACET, N_SUB, N_TEAM, 2, VDEV), 1.0, 6.0, ((0, 4), (2, 4))),
        "weights": jnp.clip(jnp.exp(math.log(3.0) - 2.306499 * jax.random.uniform(splits[6], (N_FACET, N_SUB, N_TEAM, VDEV), jnp.float32) ** block_scale(splits[6], (N_FACET, N_SUB, N_TEAM, VDEV), ((0, 4), (2, 4)), -0.2, 0.2)), 0.29882812, 3.0).astype(jnp.bfloat16),
        "counts": draw_counts(jax.random.fold_in(splits[8], 71), 0),
    }


TWO_PI = 2.0 * math.pi
HIGHEST = lax.Precision.HIGHEST

def angles(left_ints, right_ints, period):
    return (left_ints * right_ints % period).astype(jnp.float32) * (TWO_PI / period)

def rounded(values_in):
    return lax.optimization_barrier(values_in.astype(jnp.bfloat16)).astype(jnp.float32)

def transform_tables():
    columns = jnp.arange(L, dtype=jnp.int32)
    frequency = jnp.arange(M, dtype=jnp.int32)
    angle_grid = angles(columns[:, None], frequency[None, :], L)
    cos_part = jnp.cos(angle_grid)
    sin_part = jnp.sin(angle_grid)
    spec_re = (cos_part / math.sqrt(L)).astype(jnp.bfloat16)
    spec_im = (-sin_part / math.sqrt(L)).astype(jnp.bfloat16)
    forward = jnp.concatenate([jnp.concatenate([spec_re, spec_im], 1), jnp.concatenate([-spec_im, spec_re], 1)], 0)
    back_re = (cos_part.T / math.sqrt(M)).astype(jnp.bfloat16)
    back_im = (sin_part.T / math.sqrt(M)).astype(jnp.bfloat16)
    backward = jnp.concatenate([jnp.concatenate([back_re, back_im], 1), jnp.concatenate([-back_im, back_re], 1)], 0)
    return (forward, backward)

def subgrid_table(size_sub):
    freq_ids = jnp.arange(M, dtype=jnp.int32)
    cell_ids = jnp.arange(size_sub, dtype=jnp.int32)
    angle_grid = angles(freq_ids[:, None], cell_ids[None, :], size_sub)
    factor = 1.0 / math.sqrt(M)
    return (jnp.cos(angle_grid) * factor, jnp.sin(angle_grid) * factor)

def facet_phase(row_ids, facet_offsets):
    col_ids = jnp.arange(M, dtype=jnp.int32)
    along_rows = row_ids[:, None] * facet_offsets[None, :, 0] % L
    along_cols = col_ids[None, :] * facet_offsets[:, 1:2] % L
    angle_grid = ((along_rows[:, :, None] + along_cols[None, :, :]) % L).astype(jnp.float32) * (TWO_PI / L)
    return (jnp.cos(angle_grid), jnp.sin(angle_grid))

def hdot(left, right):
    return jnp.dot(left, right, precision=HIGHEST, preferred_element_type=jnp.float32)

def to_image(assembled, k_re, k_im):
    grid_re = assembled[:, 0]
    grid_im = assembled[:, 1]
    temp_re = hdot(k_re.T, grid_re) - hdot(k_im.T, grid_im)
    temp_im = hdot(k_re.T, grid_im) + hdot(k_im.T, grid_re)
    image_re = hdot(temp_re, k_re) - hdot(temp_im, k_im)
    image_im = hdot(temp_re, k_im) + hdot(temp_im, k_re)
    return (image_re, image_im)

def to_return(grid, weight_map, k_re, k_im):
    size_sub = weight_map.shape[0]
    grid_re = grid[:, :size_sub] * weight_map / size_sub
    grid_im = grid[:, size_sub:] * weight_map / size_sub
    temp_re = hdot(k_re, grid_re) + hdot(k_im, grid_im)
    temp_im = hdot(k_re, grid_im) - hdot(k_im, grid_re)
    out_re = hdot(temp_re, k_re.T) + hdot(temp_im, k_im.T)
    out_im = hdot(temp_im, k_re.T) - hdot(temp_re, k_im.T)
    return jnp.stack([out_re, out_im], 1)

def degrid_block(weighted, cell_pair, observed_pair, weight, live):
    size_sub = weighted.shape[1]
    block_len = cell_pair.shape[1]
    index = jnp.arange(size_sub, dtype=jnp.int32)
    row_angle = angles(cell_pair[0][:, None], index[None, :], 4 * size_sub)
    col_angle = angles(cell_pair[1][:, None], index[None, :], 4 * size_sub)
    cos_rows = rounded(jnp.cos(row_angle))
    sin_rows = rounded(jnp.sin(row_angle))
    cos_cols = rounded(jnp.cos(col_angle))
    sin_cols = rounded(jnp.sin(col_angle))
    col_stack = jnp.concatenate([cos_cols, sin_cols], 0)
    products = jnp.einsum('jk,ik->ji', col_stack, weighted.astype(jnp.float32), precision=HIGHEST)
    part_re = products[:block_len, :size_sub] + products[block_len:, size_sub:]
    part_im = products[:block_len, size_sub:] - products[block_len:, :size_sub]
    pred_re = lax.optimization_barrier(jnp.sum(cos_rows * part_re + sin_rows * part_im, 1)) / size_sub
    pred_im = lax.optimization_barrier(jnp.sum(cos_rows * part_im - sin_rows * part_re, 1)) / size_sub
    res_re = live * weight * (observed_pair[0] - pred_re)
    res_im = live * weight * (observed_pair[1] - pred_im)
    spread_re = rounded(res_re[:, None] * cos_cols - res_im[:, None] * sin_cols)
    spread_im = rounded(res_re[:, None] * sin_cols + res_im[:, None] * cos_cols)
    right = jnp.concatenate([jnp.concatenate([spread_re, spread_im], 1), jnp.concatenate([-spread_im, spread_re], 1)], 0)
    left = jnp.concatenate([cos_rows, sin_rows], 0)
    return jnp.einsum('ji,jk->ik', left, right, precision=HIGHEST)

def reference(facet_rows, sub_offsets, facet_offsets, aterm, cells, observed, weights, counts):
    forward, backward = transform_tables()
    k_re, k_im = subgrid_table(SG)
    norm = 1.0 / math.sqrt(N_FACET)
    columns = jnp.arange(L, dtype=jnp.int32)
    row_ids = jnp.arange(R, dtype=jnp.int32)
    out_ids = jnp.arange(M, dtype=jnp.int32)
    slot_ids = jnp.arange(VDEV, dtype=jnp.int32)
    facet_re = facet_rows[:, 0].astype(jnp.float32)
    facet_im = facet_rows[:, 1].astype(jnp.float32)
    phase_cos, phase_sin = facet_phase(out_ids, facet_offsets)

    def one_subgrid(total, subgrid):
        owner = subgrid // N_SUB
        side = subgrid % N_SUB
        mod_angle = angles(sub_offsets[subgrid, 1], columns, L)
        mod_cos = jnp.cos(mod_angle)[None, None, :]
        mod_sin = jnp.sin(mod_angle)[None, None, :]
        mod_re = (facet_re * mod_cos + facet_im * mod_sin).astype(jnp.bfloat16)
        mod_im = (facet_im * mod_cos - facet_re * mod_sin).astype(jnp.bfloat16)
        stacked = jnp.concatenate([mod_re, mod_im], 2).reshape(N_FACET * R, 2 * L)
        spectrum = jnp.dot(stacked, forward, preferred_element_type=jnp.float32).reshape(N_FACET, R, 2, M)
        w_angle = angles(out_ids[:, None] + sub_offsets[subgrid, 0], row_ids[None, :], R)
        w_re = jnp.cos(w_angle) / math.sqrt(R)
        w_im = -jnp.sin(w_angle) / math.sqrt(R)
        con_re = jnp.einsum('pr,frm->pfm', w_re, spectrum[:, :, 0], precision=HIGHEST) - jnp.einsum('pr,frm->pfm', w_im, spectrum[:, :, 1], precision=HIGHEST)
        con_im = jnp.einsum('pr,frm->pfm', w_re, spectrum[:, :, 1], precision=HIGHEST) + jnp.einsum('pr,frm->pfm', w_im, spectrum[:, :, 0], precision=HIGHEST)
        grid_re = lax.optimization_barrier(jnp.sum(phase_cos * con_re - phase_sin * con_im, 1)) * norm
        grid_im = lax.optimization_barrier(jnp.sum(phase_cos * con_im + phase_sin * con_re, 1)) * norm
        image_re, image_im = to_image(jnp.stack([grid_re, grid_im], 1), k_re, k_im)
        weight_map = aterm[owner, side].astype(jnp.float32)
        weighted = jnp.concatenate([(weight_map * image_re).astype(jnp.bfloat16), (weight_map * image_im).astype(jnp.bfloat16)], 0)

        def one_team(team):
            live = (slot_ids < counts[owner, side, team]).astype(jnp.float32)
            return degrid_block(weighted, cells[owner, side, team], observed[owner, side, team].astype(jnp.float32), weights[owner, side, team].astype(jnp.float32), live)
        grid = lax.optimization_barrier(jnp.sum(lax.map(one_team, jnp.arange(N_TEAM, dtype=jnp.int32)), 0))
        returned = to_return(grid, weight_map, k_re, k_im)
        back_re = (phase_cos * returned[:, None, 0] + phase_sin * returned[:, None, 1]) * norm
        back_im = (phase_cos * returned[:, None, 1] - phase_sin * returned[:, None, 0]) * norm
        fold_re = jnp.einsum('pr,pfm->frm', w_re, back_re, precision=HIGHEST) + jnp.einsum('pr,pfm->frm', w_im, back_im, precision=HIGHEST)
        fold_im = jnp.einsum('pr,pfm->frm', w_re, back_im, precision=HIGHEST) - jnp.einsum('pr,pfm->frm', w_im, back_re, precision=HIGHEST)
        folded = jnp.stack([fold_re, fold_im], 2).astype(jnp.bfloat16).reshape(N_FACET * R, 2 * M)
        spectra_back = jnp.dot(folded, backward, preferred_element_type=jnp.float32).reshape(N_FACET, R, 2, L)
        update_re = spectra_back[:, :, 0] * mod_cos - spectra_back[:, :, 1] * mod_sin
        update_im = spectra_back[:, :, 1] * mod_cos + spectra_back[:, :, 0] * mod_sin
        return (total + jnp.stack([update_re, update_im], 1), None)
    start_total = jnp.zeros((N_FACET, 2, R, L), jnp.float32)
    total, _ = lax.scan(one_subgrid, start_total, jnp.arange(NS, dtype=jnp.int32))
    return total
```

```python
import functools
import math

import jax
import jax.numpy as jnp
import ml_dtypes
import numpy as np
from jax import lax
from jax.experimental import pallas as pl
from jax.experimental.pallas import tpu as pltpu
from jax.sharding import PartitionSpec as P

M = 128
TWO_PI = 2.0 * math.pi
BF = jnp.bfloat16
F32 = jnp.float32
MESH = pl.DeviceIdType.MESH


def sincos(turns, period):
    shift = period.bit_length() - 3
    quad = (turns + (1 << (shift - 1))) >> shift
    t = (turns - (quad << shift)).astype(F32) * (TWO_PI / period)
    t2 = t * t
    s = t * (1.0 + t2 * (-1.0 / 6 + t2 * (1.0 / 120 + t2 * (-1.0 / 5040))))
    c = 1.0 + t2 * (-0.5 + t2 * (1.0 / 24 + t2 * (-1.0 / 720 + t2 * (1.0 / 40320))))
    odd = (quad & 1) != 0
    cos = jnp.where(odd, s, c)
    sin = jnp.where(odd, c, s)
    cos = jnp.where(((quad + 1) & 2) != 0, -cos, cos)
    sin = jnp.where((quad & 2) != 0, -sin, sin)
    return cos, sin


def mm(left, right):
    return jnp.dot(left, right, preferred_element_type=F32)


def mm_nt(left, right):
    return lax.dot_general(left, right, (((1,), (1,)), ((), ())), preferred_element_type=F32)


def cat(parts, axis):
    return jnp.concatenate(parts, axis)


def iota(shape, dim):
    return lax.broadcasted_iota(jnp.int32, shape, dim)


def body(
    dims,
    sub_off, fac_off, counts, rows, aterm, cells, observed, weights, table, kk, kt, kb,
    out,
    phi_c, phi_s, x_buf, spec_out, got1, fold_out, got2, fold3, got3,
    send1, recv1, send2, recv2, send3, recv3,
):
    nf, nt, nb, length, size, rdev = dims
    rall = rdev * nt
    n = nf * nt
    slots = cells.shape[-1]
    period = 4 * size
    my_f = lax.axis_index("facet")
    my_t = lax.axis_index("team")
    my_b = lax.axis_index("sub")
    me = my_f * nt + my_t
    other = 1 - my_b

    def peer_of(k):
        peer = lax.rem(me + k, n)
        return peer, peer // nt, lax.rem(peer, nt)

    barrier = pltpu.get_barrier_semaphore()

    def greet(k, carry):
        _, pf, pt = peer_of(k)
        pl.semaphore_signal(
            barrier, inc=1, device_id={"facet": pf, "team": pt, "sub": my_b}, device_id_type=MESH
        )
        return carry

    lax.fori_loop(1, n, greet, 0)
    pl.semaphore_signal(
        barrier, inc=1, device_id={"facet": my_f, "team": my_t, "sub": other}, device_id_type=MESH
    )

    sub_row = iota((nb * nf, 1), 0)
    tune = jnp.zeros((nb * nf, 1), jnp.int32)
    for s in range(nf):
        tune = jnp.where(sub_row == s, sub_off[s * nb + my_b, 1], tune)
        tune = jnp.where(sub_row == nf + s, sub_off[s * nb + other, 1], tune)
    pc, ps = sincos(iota((nb * nf, length), 1) * tune, length)
    phi_c[...] = pc
    phi_s[...] = ps
    re = rows[0, 0].astype(F32)
    im = rows[0, 1].astype(F32)
    for a in range(nf):
        c = phi_c[a : a + 1, :]
        s = phi_s[a : a + 1, :]
        x_buf[a] = re * c + im * s
        x_buf[nf + a] = im * c - re * s
    x = x_buf[...].reshape(2 * nf * rdev, length).astype(BF)
    y = mm(x, table[...])
    h = nf * rdev
    spec = cat([y[:h, :M] - y[h:, M:], y[:h, M:] + y[h:, :M]], 1)
    spec_out[...] = spec.reshape(nf, rdev, 2 * M).astype(BF)

    pl.semaphore_wait(barrier, n)

    def copy1(k):
        peer, pf, pt = peer_of(k)
        return pltpu.make_async_remote_copy(
            src_ref=spec_out.at[pf],
            dst_ref=got1.at[me],
            send_sem=send1.at[k],
            recv_sem=recv1.at[me],
            device_id={"facet": pf, "team": pt, "sub": my_b},
            device_id_type=MESH,
        )

    def start1(k, carry):
        copy1(k).start()
        return carry

    lax.fori_loop(1, n, start1, 0)
    got1[me] = spec_out[my_f]

    shift_u = jnp.int32(0)
    shift_u = sub_off[my_f * nb + my_b, 0]
    step = length // rall
    scale_g = 1.0 / math.sqrt(rall * nf)
    lane = iota((1, n * rdev), 1)
    col_a = jnp.zeros((1, n * rdev), jnp.int32)
    row = iota((n * rdev, 1), 0)
    row_a = jnp.zeros((n * rdev, 1), jnp.int32)
    row_c = jnp.zeros((n * rdev, 1), jnp.int32)
    for f in range(nf):
        col_a = jnp.where(lane // rall == f, fac_off[f, 0], col_a)
        row_a = jnp.where(row // rall == f, fac_off[f, 0], row_a)
        row_c = jnp.where(row // rall == f, fac_off[f, 1], row_c)
    p0 = iota((M, n * rdev), 0)
    gc, gs = sincos(p0 * col_a - (p0 + shift_u) * (lane % rall * step), length)
    gc = (gc * scale_g).astype(BF)
    gs = (gs * scale_g).astype(BF)
    a_mat = mm(kt[...], cat([cat([gc, gs], 1), cat([-gs, gc], 1)], 0)).astype(BF)
    p1 = iota((n * rdev, M), 1)
    hc, hs = sincos(p1 * row_a - (p1 + shift_u) * (row % rall * step), length)
    at = mm(cat([hc * scale_g, hs * scale_g], 1).astype(BF), kk[...])
    ah = cat([at[:, :size], -at[:, size:]], 1).astype(BF)
    ec, es = sincos(p1 * row_c, length)
    own_scale = math.sqrt(length / M) / size
    own_c, own_s = sincos(iota((rdev, M), 1) * fac_off[my_f, 1], length)
    own_c = own_c * own_scale
    own_s = own_s * own_scale
    pair = cells[0, my_b, 0]
    index = iota((size, slots), 0)
    rc, rs = sincos(index * pair[0:1, :], period)
    rc = rc.astype(BF)
    rs = rs.astype(BF)
    cc, cs = sincos(index * pair[1:2, :], period)
    cc = cc.astype(BF)
    cs = cs.astype(BF)
    col_w = cat([cat([cc, -cs], 1), cat([cs, cc], 1)], 0)
    left = cat([rc, rs], 1)
    amap = aterm[0, my_b].astype(F32)
    amap = cat([amap, amap], 1)
    obs = observed[0, my_b, 0].astype(F32)
    live = iota((1, slots), 1) < counts[my_f, my_b, my_t]
    wt = jnp.where(live, weights[0, my_b].astype(F32), 0.0)

    def take1(k, carry):
        peer, _, _ = peer_of(k)
        pltpu.make_async_copy(got1.at[peer], got1.at[peer], recv1.at[peer]).wait()
        return carry

    lax.fori_loop(1, n, take1, 0)
    sp = got1[...].astype(F32).reshape(n * rdev, 2 * M)
    sr = sp[:, :M]
    si = sp[:, M:]
    turned = cat([sr * ec - si * es, sr * es + si * ec], 1).astype(BF)
    t = mm(turned, kk[...]).astype(BF)
    tr = t[:, :size]
    ti = t[:, size:]
    image = mm(a_mat, cat([t, cat([-ti, tr], 1)], 0))
    weighted = (amap * image).astype(BF)
    z = mm(weighted, col_w)
    zr = z[:, :slots]
    zi = z[:, slots:]
    rcf = rc.astype(F32)
    rsf = rs.astype(F32)
    pred_re = jnp.sum(rcf * zr + rsf * zi, 0, keepdims=True) * (1.0 / size)
    pred_im = jnp.sum(rcf * zi - rsf * zr, 0, keepdims=True) * (1.0 / size)
    res_re = wt * (obs[0:1, :] - pred_re)
    res_im = wt * (obs[1:2, :] - pred_im)
    ccf = cc.astype(F32)
    csf = cs.astype(F32)
    s_re = (res_re * ccf - res_im * csf).astype(BF)
    s_im = (res_re * csf + res_im * ccf).astype(BF)
    grid = mm_nt(left, cat([cat([s_re, -s_im], 1), cat([s_im, s_re], 1)], 0))
    v = (amap * grid).astype(BF)
    u = mm(v, kb[...]).astype(BF)
    ur = u[:, :M]
    ui = u[:, M:]
    part = mm(ah, cat([u, cat([-ui, ur], 1)], 0))
    fold_out[...] = part.reshape(n, rdev, 2 * M).astype(BF)

    def copy2(k):
        peer, pf, pt = peer_of(k)
        return pltpu.make_async_remote_copy(
            src_ref=fold_out.at[peer],
            dst_ref=got2.at[me],
            send_sem=send2.at[k],
            recv_sem=recv2.at[me],
            device_id={"facet": pf, "team": pt, "sub": my_b},
            device_id_type=MESH,
        )

    def start2(k, carry):
        copy2(k).start()
        return carry

    lax.fori_loop(1, n, start2, 0)
    got2[me] = fold_out[me]

    def take2(k, carry):
        peer, _, _ = peer_of(k)
        pltpu.make_async_copy(got2.at[peer], got2.at[peer], recv2.at[peer]).wait()
        return carry

    lax.fori_loop(1, n, take2, 0)
    parts = got2[...].astype(F32).reshape(nf, nt, rdev, 2 * M)
    folded = jnp.sum(parts, 1)
    fr = folded[:, :, :M]
    fi = folded[:, :, M:]
    oc = own_c[None]
    os_ = own_s[None]
    fold3[...] = cat([fr * oc + fi * os_, fi * oc - fr * os_], 2).astype(BF)
    copy3 = pltpu.make_async_remote_copy(
        src_ref=fold3,
        dst_ref=got3,
        send_sem=send3,
        recv_sem=recv3,
        device_id={"facet": my_f, "team": my_t, "sub": other},
        device_id_type=MESH,
    )
    copy3.start()
    half = length // nb
    base = pl.multiple_of(my_b * half, 128)
    back = table[pl.ds(base, half), :]

    def update(stack, first):
        stack = stack.astype(F32).reshape(nf * rdev, 2 * M)
        turned = cat([stack[:, M:], -stack[:, :M]], 1)
        pre = mm_nt(cat([stack, turned], 0).astype(BF), back)
        tot_re = tot_im = None
        for a in range(nf):
            c = phi_c[first + a : first + a + 1, pl.ds(base, half)]
            s = phi_s[first + a : first + a + 1, pl.ds(base, half)]
            pr = pre[a * rdev : (a + 1) * rdev]
            pi = pre[h + a * rdev : h + (a + 1) * rdev]
            add_re = pr * c - pi * s
            add_im = pi * c + pr * s
            tot_re = add_re if tot_re is None else tot_re + add_re
            tot_im = add_im if tot_im is None else tot_im + add_im
        return tot_re, tot_im

    own_re, own_im = update(fold3[...], 0)
    copy3.wait_recv()
    oth_re, oth_im = update(got3[...], nf)
    out[0, 0] = own_re + oth_re
    out[0, 1] = own_im + oth_im

    def finish(k, carry):
        copy1(k).wait_send()
        copy2(k).wait_send()
        return carry

    lax.fori_loop(1, n, finish, 0)
    copy3.wait_send()


def tables(length, size):
    turn = np.arange(length)[:, None] * np.arange(M)[None, :] % length
    angle = turn * (TWO_PI / length)
    forward = np.concatenate([np.cos(angle), -np.sin(angle)], 1) / math.sqrt(length)
    angle = (np.arange(M)[:, None] * np.arange(size)[None, :] % size) * (TWO_PI / size)
    kc = np.cos(angle) / math.sqrt(M)
    ks = np.sin(angle) / math.sqrt(M)
    kk = np.block([[kc, ks], [-ks, kc]])
    kt = np.concatenate([kc.T, ks.T], 1)
    kb = np.block([[kc.T, -ks.T], [ks.T, kc.T]])
    return [np.asarray(v, np.float32).astype(ml_dtypes.bfloat16) for v in (forward, kk, kt, kb)]


def local(facet_rows, sub_offsets, facet_offsets, aterm, cells, observed, weights, counts):
    nf = lax.axis_size("facet")
    nt = lax.axis_size("team")
    nb = lax.axis_size("sub")
    rdev, length = facet_rows.shape[2:]
    size = aterm.shape[-1]
    n = nf * nt
    dims = (nf, nt, nb, length, size, rdev)
    consts = [jnp.asarray(v) for v in tables(length, size)]
    vm = pl.BlockSpec(memory_space=pltpu.VMEM)
    sm = pl.BlockSpec(memory_space=pltpu.SMEM)
    dma = pltpu.SemaphoreType.DMA
    return pl.pallas_call(
        functools.partial(body, dims),
        out_shape=jax.ShapeDtypeStruct((1, 2, rdev, length // nb), F32),
        in_specs=[sm] * 3 + [vm] * 9,
        out_specs=vm,
        scratch_shapes=[
            pltpu.VMEM((nb * nf, length), F32),
            pltpu.VMEM((nb * nf, length), F32),
            pltpu.VMEM((2 * nf, rdev, length), F32),
            pltpu.VMEM((nf, rdev, 2 * M), BF),
            pltpu.VMEM((n, rdev, 2 * M), BF),
            pltpu.VMEM((n, rdev, 2 * M), BF),
            pltpu.VMEM((n, rdev, 2 * M), BF),
            pltpu.VMEM((nf, rdev, 2 * M), BF),
            pltpu.VMEM((nf, rdev, 2 * M), BF),
            dma((n,)), dma((n,)), dma((n,)), dma((n,)), dma, dma,
        ],
        compiler_params=pltpu.CompilerParams(collective_id=0, has_side_effects=True),
    )(sub_offsets, facet_offsets, counts, facet_rows, aterm, cells, observed, weights, *consts)


def solution(mesh):
    placed = (
        P("facet", None, "team", None),
        P(),
        P(),
        P("facet", None, None, None),
        P("facet", None, "team", None, None),
        P("facet", None, "team", None, None),
        P("facet", None, "team", None),
        P(),
    )
    return jax.shard_map(
        local,
        mesh=mesh,
        in_specs=placed,
        out_specs=P("facet", None, "team", "sub"),
        check_vma=False,
    )
```

```python
import functools
import math

import jax
import jax.numpy as jnp
import ml_dtypes
import numpy as np
from jax import lax
from jax.experimental import pallas as pl
from jax.experimental.pallas import tpu as pltpu
from jax.sharding import PartitionSpec as P

M = 128
TWO_PI = 2.0 * math.pi
BF = jnp.bfloat16
F32 = jnp.float32
MESH = pl.DeviceIdType.MESH


def sincos(turns, period):
    shift = period.bit_length() - 3
    quad = (turns + (1 << (shift - 1))) >> shift
    t = (turns - (quad << shift)).astype(F32) * (TWO_PI / period)
    t2 = t * t
    s = t * (1.0 + t2 * (-1.0 / 6 + t2 * (1.0 / 120 + t2 * (-1.0 / 5040))))
    c = 1.0 + t2 * (-0.5 + t2 * (1.0 / 24 + t2 * (-1.0 / 720 + t2 * (1.0 / 40320))))
    odd = (quad & 1) != 0
    cos = jnp.where(odd, s, c)
    sin = jnp.where(odd, c, s)
    cos = jnp.where(((quad + 1) & 2) != 0, -cos, cos)
    sin = jnp.where((quad & 2) != 0, -sin, sin)
    return cos, sin


def mm(left, right):
    return jnp.dot(left, right, preferred_element_type=F32)


def mm_nt(left, right):
    return lax.dot_general(left, right, (((1,), (1,)), ((), ())), preferred_element_type=F32)


def cat(parts, axis):
    return jnp.concatenate(parts, axis)


def iota(shape, dim):
    return lax.broadcasted_iota(jnp.int32, shape, dim)


def body(
    dims,
    *refs,
):
    ins = refs[:12]
    out = refs[12]
    bufs = refs[13:25]
    (
    phi_c, phi_s, x_buf, spec_out, got1, fold_out, got2, fold3, got3,
    send1, recv1, send2, recv2, send3, recv3, in_sem, out_buf, out_sem,
    ) = refs[25:]
    sub_off, fac_off, counts, rows, aterm, cells, observed, weights, table, kk, kt, kb = bufs
    nf, nt, nb, length, size, rdev = dims
    rall = rdev * nt
    n = nf * nt
    slots = cells.shape[-1]
    period = 4 * size
    my_f = lax.axis_index("facet")
    my_t = lax.axis_index("team")
    my_b = lax.axis_index("sub")
    me = my_f * nt + my_t
    other = 1 - my_b

    def peer_of(k):
        peer = lax.rem(me + k, n)
        return peer, peer // nt, lax.rem(peer, nt)

    barrier = pltpu.get_barrier_semaphore()

    def greet(k, carry):
        _, pf, pt = peer_of(k)
        pl.semaphore_signal(
            barrier, inc=1, device_id={"facet": pf, "team": pt, "sub": my_b}, device_id_type=MESH
        )
        return carry

    lax.fori_loop(1, n, greet, 0)
    pl.semaphore_signal(
        barrier, inc=1, device_id={"facet": my_f, "team": my_t, "sub": other}, device_id_type=MESH
    )

    fetches = [pltpu.make_async_copy(ins[i], bufs[i], in_sem.at[i]) for i in range(12)]
    for i in (0, 3, 8, 1, 5, 10, 9, 4, 2, 6, 7, 11):
        fetches[i].start()
    fetches[0].wait()

    sub_row = iota((nb * nf, 1), 0)
    tune = jnp.zeros((nb * nf, 1), jnp.int32)
    for s in range(nf):
        tune = jnp.where(sub_row == s, sub_off[1, s * nb + my_b], tune)
        tune = jnp.where(sub_row == nf + s, sub_off[1, s * nb + other], tune)
    pc, ps = sincos(iota((nb * nf, length), 1) * tune, length)
    phi_c[...] = pc
    phi_s[...] = ps
    fetches[3].wait()
    re = rows[0, 0].astype(F32)
    im = rows[0, 1].astype(F32)
    for a in range(nf):
        c = phi_c[a : a + 1, :]
        s = phi_s[a : a + 1, :]
        x_buf[a] = re * c + im * s
        x_buf[nf + a] = im * c - re * s
    x = x_buf[...].reshape(2 * nf * rdev, length).astype(BF)
    fetches[8].wait()
    y = mm(x, table[...])
    h = nf * rdev
    spec = cat([y[:h, :M] - y[h:, M:], y[:h, M:] + y[h:, :M]], 1)
    spec_out[...] = spec.reshape(nf, rdev, 2 * M).astype(BF)

    pl.semaphore_wait(barrier, n)

    def copy1(k):
        peer, pf, pt = peer_of(k)
        return pltpu.make_async_remote_copy(
            src_ref=spec_out.at[pf],
            dst_ref=got1.at[me],
            send_sem=send1.at[k],
            recv_sem=recv1.at[me],
            device_id={"facet": pf, "team": pt, "sub": my_b},
            device_id_type=MESH,
        )

    def start1(k, carry):
        copy1(k).start()
        return carry

    lax.fori_loop(1, n, start1, 0)
    got1[me] = spec_out[my_f]

    for i in (1, 5, 10, 9, 4, 2, 6, 7, 11):
        fetches[i].wait()
    shift_u = sub_off[0, my_f * nb + my_b]
    step = length // rall
    scale_g = 1.0 / math.sqrt(rall * nf)
    lane = iota((1, n * rdev), 1)
    col_a = jnp.zeros((1, n * rdev), jnp.int32)
    row = iota((n * rdev, 1), 0)
    row_a = jnp.zeros((n * rdev, 1), jnp.int32)
    row_c = jnp.zeros((n * rdev, 1), jnp.int32)
    for f in range(nf):
        col_a = jnp.where(lane // rall == f, fac_off[0, f], col_a)
        row_a = jnp.where(row // rall == f, fac_off[0, f], row_a)
        row_c = jnp.where(row // rall == f, fac_off[1, f], row_c)
    p0 = iota((M, n * rdev), 0)
    gc, gs = sincos(p0 * col_a - (p0 + shift_u) * (lane % rall * step), length)
    gc = (gc * scale_g).astype(BF)
    gs = (gs * scale_g).astype(BF)
    a_mat = mm(kt[...], cat([cat([gc, gs], 1), cat([-gs, gc], 1)], 0)).astype(BF)
    p1 = iota((n * rdev, M), 1)
    hc, hs = sincos(p1 * row_a - (p1 + shift_u) * (row % rall * step), length)
    at = mm(cat([hc * scale_g, hs * scale_g], 1).astype(BF), kk[...])
    ah = cat([at[:, :size], -at[:, size:]], 1).astype(BF)
    ec, es = sincos(p1 * row_c, length)
    own_scale = math.sqrt(length / M) / size
    own_c, own_s = sincos(iota((rdev, M), 1) * fac_off[1, my_f], length)
    own_c = own_c * own_scale
    own_s = own_s * own_scale
    pair = cells[0, my_b, 0]
    index = iota((size, slots), 0)
    rc, rs = sincos(index * pair[0:1, :], period)
    rc = rc.astype(BF)
    rs = rs.astype(BF)
    cc, cs = sincos(index * pair[1:2, :], period)
    cc = cc.astype(BF)
    cs = cs.astype(BF)
    col_w = cat([cat([cc, -cs], 1), cat([cs, cc], 1)], 0)
    left = cat([rc, rs], 1)
    amap = aterm[0, my_b].astype(F32)
    amap = cat([amap, amap], 1)
    obs = observed[0, my_b, 0].astype(F32)
    live = iota((1, slots), 1) < counts[my_f, my_b, my_t]
    all_wt = weights[0, 0].astype(F32)
    own_wt = jnp.where(my_b == 0, all_wt[0:1, :], all_wt[1:2, :])
    wt = jnp.where(live, own_wt, 0.0)

    def take1(k, carry):
        peer, _, _ = peer_of(k)
        pltpu.make_async_copy(got1.at[peer], got1.at[peer], recv1.at[peer]).wait()
        return carry

    lax.fori_loop(1, n, take1, 0)
    sp = got1[...].astype(F32).reshape(n * rdev, 2 * M)
    sr = sp[:, :M]
    si = sp[:, M:]
    turned = cat([sr * ec - si * es, sr * es + si * ec], 1).astype(BF)
    t = mm(turned, kk[...]).astype(BF)
    tr = t[:, :size]
    ti = t[:, size:]
    image = mm(a_mat, cat([t, cat([-ti, tr], 1)], 0))
    weighted = (amap * image).astype(BF)
    z = mm(weighted, col_w)
    zr = z[:, :slots]
    zi = z[:, slots:]
    rcf = rc.astype(F32)
    rsf = rs.astype(F32)
    pred_re = jnp.sum(rcf * zr + rsf * zi, 0, keepdims=True) * (1.0 / size)
    pred_im = jnp.sum(rcf * zi - rsf * zr, 0, keepdims=True) * (1.0 / size)
    res_re = wt * (obs[0:1, :] - pred_re)
    res_im = wt * (obs[1:2, :] - pred_im)
    ccf = cc.astype(F32)
    csf = cs.astype(F32)
    s_re = (res_re * ccf - res_im * csf).astype(BF)
    s_im = (res_re * csf + res_im * ccf).astype(BF)
    grid = mm_nt(left, cat([cat([s_re, -s_im], 1), cat([s_im, s_re], 1)], 0))
    v = (amap * grid).astype(BF)
    u = mm(v, kb[...]).astype(BF)
    ur = u[:, :M]
    ui = u[:, M:]
    part = mm(ah, cat([u, cat([-ui, ur], 1)], 0))
    fold_out[...] = part.reshape(n, rdev, 2 * M).astype(BF)

    def copy2(k):
        peer, pf, pt = peer_of(k)
        return pltpu.make_async_remote_copy(
            src_ref=fold_out.at[peer],
            dst_ref=got2.at[me],
            send_sem=send2.at[k],
            recv_sem=recv2.at[me],
            device_id={"facet": pf, "team": pt, "sub": my_b},
            device_id_type=MESH,
        )

    def start2(k, carry):
        copy2(k).start()
        return carry

    lax.fori_loop(1, n, start2, 0)
    got2[me] = fold_out[me]

    def take2(k, carry):
        peer, _, _ = peer_of(k)
        pltpu.make_async_copy(got2.at[peer], got2.at[peer], recv2.at[peer]).wait()
        return carry

    lax.fori_loop(1, n, take2, 0)
    parts = got2[...].astype(F32).reshape(nf, nt, rdev, 2 * M)
    folded = jnp.sum(parts, 1)
    fr = folded[:, :, :M]
    fi = folded[:, :, M:]
    oc = own_c[None]
    os_ = own_s[None]
    fold3[...] = cat([fr * oc + fi * os_, fi * oc - fr * os_], 2).astype(BF)
    copy3 = pltpu.make_async_remote_copy(
        src_ref=fold3,
        dst_ref=got3,
        send_sem=send3,
        recv_sem=recv3,
        device_id={"facet": my_f, "team": my_t, "sub": other},
        device_id_type=MESH,
    )
    copy3.start()
    half = length // nb
    base = pl.multiple_of(my_b * half, 128)
    back = table[pl.ds(base, half), :]

    def update(stack, first):
        stack = stack.astype(F32).reshape(nf * rdev, 2 * M)
        turned = cat([stack[:, M:], -stack[:, :M]], 1)
        pre = mm_nt(cat([stack, turned], 0).astype(BF), back)
        tot_re = tot_im = None
        for a in range(nf):
            c = phi_c[first + a : first + a + 1, pl.ds(base, half)]
            s = phi_s[first + a : first + a + 1, pl.ds(base, half)]
            pr = pre[a * rdev : (a + 1) * rdev]
            pi = pre[h + a * rdev : h + (a + 1) * rdev]
            add_re = pr * c - pi * s
            add_im = pi * c + pr * s
            tot_re = add_re if tot_re is None else tot_re + add_re
            tot_im = add_im if tot_im is None else tot_im + add_im
        return tot_re, tot_im

    own_re, own_im = update(fold3[...], 0)
    copy3.wait_recv()
    oth_re, oth_im = update(got3[...], nf)
    out_buf[0, 0] = own_re + oth_re
    out_buf[0, 1] = own_im + oth_im
    put = pltpu.make_async_copy(out_buf, out, out_sem)
    put.start()

    def finish(k, carry):
        copy1(k).wait_send()
        copy2(k).wait_send()
        return carry

    lax.fori_loop(1, n, finish, 0)
    copy3.wait_send()
    put.wait()


def tables(length, size):
    turn = np.arange(length)[:, None] * np.arange(M)[None, :] % length
    angle = turn * (TWO_PI / length)
    forward = np.concatenate([np.cos(angle), -np.sin(angle)], 1) / math.sqrt(length)
    angle = (np.arange(M)[:, None] * np.arange(size)[None, :] % size) * (TWO_PI / size)
    kc = np.cos(angle) / math.sqrt(M)
    ks = np.sin(angle) / math.sqrt(M)
    kk = np.block([[kc, ks], [-ks, kc]])
    kt = np.concatenate([kc.T, ks.T], 1)
    kb = np.block([[kc.T, -ks.T], [ks.T, kc.T]])
    return [np.asarray(v, np.float32).astype(ml_dtypes.bfloat16) for v in (forward, kk, kt, kb)]


def local(facet_rows, sub_offsets, facet_offsets, aterm, cells, observed, weights, counts):
    nf = lax.axis_size("facet")
    nt = lax.axis_size("team")
    nb = lax.axis_size("sub")
    rdev, length = facet_rows.shape[2:]
    size = aterm.shape[-1]
    n = nf * nt
    dims = (nf, nt, nb, length, size, rdev)
    consts = [jnp.asarray(v) for v in tables(length, size)]
    hbm = pl.BlockSpec(memory_space=pltpu.HBM)
    operands = [
        sub_offsets.T, facet_offsets.T, counts, facet_rows, aterm, cells, observed,
        weights.transpose(0, 2, 1, 3), *consts,
    ]
    dma = pltpu.SemaphoreType.DMA
    return pl.pallas_call(
        functools.partial(body, dims),
        out_shape=jax.ShapeDtypeStruct((1, 2, rdev, length // nb), F32),
        in_specs=[hbm] * 12,
        out_specs=pl.BlockSpec(memory_space=pl.ANY),
        scratch_shapes=[
            *[pltpu.SMEM(v.shape, v.dtype) for v in operands[:3]],
            *[pltpu.VMEM(v.shape, v.dtype) for v in operands[3:]],
            pltpu.VMEM((nb * nf, length), F32),
            pltpu.VMEM((nb * nf, length), F32),
            pltpu.VMEM((2 * nf, rdev, length), F32),
            pltpu.VMEM((nf, rdev, 2 * M), BF),
            pltpu.VMEM((n, rdev, 2 * M), BF),
            pltpu.VMEM((n, rdev, 2 * M), BF),
            pltpu.VMEM((n, rdev, 2 * M), BF),
            pltpu.VMEM((nf, rdev, 2 * M), BF),
            pltpu.VMEM((nf, rdev, 2 * M), BF),
            dma((n,)), dma((n,)), dma((n,)), dma((n,)), dma, dma, dma((12,)),
            pltpu.VMEM((1, 2, rdev, length // nb), F32),
            dma,
        ],
        compiler_params=pltpu.CompilerParams(
            collective_id=0, has_side_effects=True
        ),
    )(*operands)


def solution(mesh):
    placed = (
        P("facet", None, "team", None),
        P(),
        P(),
        P("facet", None, None, None),
        P("facet", None, "team", None, None),
        P("facet", None, "team", None, None),
        P("facet", None, "team", None),
        P(),
    )
    return jax.shard_map(
        local,
        mesh=mesh,
        in_specs=placed,
        out_specs=P("facet", None, "team", "sub"),
        check_vma=False,
    )
```

```python
import functools
import math

import jax
import jax.numpy as jnp
import ml_dtypes
import numpy as np
from jax import lax
from jax.experimental import pallas as pl
from jax.experimental.pallas import tpu as pltpu
from jax.sharding import PartitionSpec as P

M = 128
TWO_PI = 2.0 * math.pi
BF = jnp.bfloat16
F32 = jnp.float32
MESH = pl.DeviceIdType.MESH


def sincos(turns, period):
    shift = period.bit_length() - 3
    quad = (turns + (1 << (shift - 1))) >> shift
    t = (turns - (quad << shift)).astype(F32) * (TWO_PI / period)
    t2 = t * t
    s = t * (1.0 + t2 * (-1.0 / 6 + t2 * (1.0 / 120 + t2 * (-1.0 / 5040))))
    c = 1.0 + t2 * (-0.5 + t2 * (1.0 / 24 + t2 * (-1.0 / 720 + t2 * (1.0 / 40320))))
    odd = (quad & 1) != 0
    cos = jnp.where(odd, s, c)
    sin = jnp.where(odd, c, s)
    cos = jnp.where(((quad + 1) & 2) != 0, -cos, cos)
    sin = jnp.where((quad & 2) != 0, -sin, sin)
    return cos, sin


def mm(left, right):
    return jnp.dot(left, right, preferred_element_type=F32)


def mm_nt(left, right):
    return lax.dot_general(left, right, (((1,), (1,)), ((), ())), preferred_element_type=F32)


def cat(parts, axis):
    return jnp.concatenate(parts, axis)


def iota(shape, dim):
    return lax.broadcasted_iota(jnp.int32, shape, dim)


def body(
    dims,
    *refs,
):
    ins = refs[:12]
    out = refs[12]
    bufs = refs[13:25]
    (
    phi_c, phi_s, x_buf, spec_out, got1, fold_out, got2, fold3, got3,
    send1, recv1, send2, recv2, send3, recv3, in_sem,
    ) = refs[25:]
    sub_off, fac_off, counts, rows, aterm, cells, observed, weights, table, kk, kt, kb = bufs
    nf, nt, nb, length, size, rdev = dims
    rall = rdev * nt
    n = nf * nt
    slots = cells.shape[-1]
    period = 4 * size
    my_f = lax.axis_index("facet")
    my_t = lax.axis_index("team")
    my_b = lax.axis_index("sub")
    me = my_f * nt + my_t
    other = 1 - my_b

    def peer_of(k):
        peer = lax.rem(me + k, n)
        return peer, peer // nt, lax.rem(peer, nt)

    barrier = pltpu.get_barrier_semaphore()

    def greet(k, carry):
        _, pf, pt = peer_of(k)
        pl.semaphore_signal(
            barrier, inc=1, device_id={"facet": pf, "team": pt, "sub": my_b}, device_id_type=MESH
        )
        return carry

    lax.fori_loop(1, n, greet, 0)
    pl.semaphore_signal(
        barrier, inc=1, device_id={"facet": my_f, "team": my_t, "sub": other}, device_id_type=MESH
    )

    fetches = [pltpu.make_async_copy(ins[i], bufs[i], in_sem.at[i]) for i in range(12)]
    for i in (0, 3, 8, 1, 5, 10, 9, 4, 2, 6, 7, 11):
        fetches[i].start()
    fetches[0].wait()

    sub_row = iota((nb * nf, 1), 0)
    tune = jnp.zeros((nb * nf, 1), jnp.int32)
    for s in range(nf):
        tune = jnp.where(sub_row == s, sub_off[1, s * nb + my_b], tune)
        tune = jnp.where(sub_row == nf + s, sub_off[1, s * nb + other], tune)
    pc, ps = sincos(iota((nb * nf, length), 1) * tune, length)
    phi_c[...] = pc
    phi_s[...] = ps
    fetches[3].wait()
    re = rows[0, 0].astype(F32)
    im = rows[0, 1].astype(F32)
    for a in range(nf):
        c = phi_c[a : a + 1, :]
        s = phi_s[a : a + 1, :]
        x_buf[a] = re * c + im * s
        x_buf[nf + a] = im * c - re * s
    x = x_buf[...].reshape(2 * nf * rdev, length).astype(BF)
    fetches[8].wait()
    y = mm(x, table[...])
    h = nf * rdev
    spec = cat([y[:h, :M] - y[h:, M:], y[:h, M:] + y[h:, :M]], 1)
    spec_out[...] = spec.reshape(nf, rdev, 2 * M).astype(BF)

    pl.semaphore_wait(barrier, n)

    def copy1(k):
        peer, pf, pt = peer_of(k)
        return pltpu.make_async_remote_copy(
            src_ref=spec_out.at[pf],
            dst_ref=got1.at[me],
            send_sem=send1.at[k],
            recv_sem=recv1.at[me],
            device_id={"facet": pf, "team": pt, "sub": my_b},
            device_id_type=MESH,
        )

    def start1(k, carry):
        copy1(k).start()
        return carry

    lax.fori_loop(1, n, start1, 0)
    got1[me] = spec_out[my_f]

    for i in (1, 5, 10, 9, 4, 2, 6, 7, 11):
        fetches[i].wait()
    shift_u = sub_off[0, my_f * nb + my_b]
    step = length // rall
    scale_g = 1.0 / math.sqrt(rall * nf)
    lane = iota((1, n * rdev), 1)
    col_a = jnp.zeros((1, n * rdev), jnp.int32)
    row = iota((n * rdev, 1), 0)
    row_a = jnp.zeros((n * rdev, 1), jnp.int32)
    row_c = jnp.zeros((n * rdev, 1), jnp.int32)
    for f in range(nf):
        col_a = jnp.where(lane // rall == f, fac_off[0, f], col_a)
        row_a = jnp.where(row // rall == f, fac_off[0, f], row_a)
        row_c = jnp.where(row // rall == f, fac_off[1, f], row_c)
    p0 = iota((M, n * rdev), 0)
    gc, gs = sincos(p0 * col_a - (p0 + shift_u) * (lane % rall * step), length)
    gc = (gc * scale_g).astype(BF)
    gs = (gs * scale_g).astype(BF)
    a_mat = mm(kt[...], cat([cat([gc, gs], 1), cat([-gs, gc], 1)], 0)).astype(BF)
    p1 = iota((n * rdev, M), 1)
    hc, hs = sincos(p1 * row_a - (p1 + shift_u) * (row % rall * step), length)
    at = mm(cat([hc * scale_g, hs * scale_g], 1).astype(BF), kk[...])
    ah = cat([at[:, :size], -at[:, size:]], 1).astype(BF)
    ec, es = sincos(p1 * row_c, length)
    own_scale = math.sqrt(length / M) / size
    own_c, own_s = sincos(iota((rdev, M), 1) * fac_off[1, my_f], length)
    own_c = own_c * own_scale
    own_s = own_s * own_scale
    pair = cells[0, my_b, 0]
    index = iota((size, slots), 0)
    rc, rs = sincos(index * pair[0:1, :], period)
    rc = rc.astype(BF)
    rs = rs.astype(BF)
    cc, cs = sincos(index * pair[1:2, :], period)
    cc = cc.astype(BF)
    cs = cs.astype(BF)
    col_w = cat([cat([cc, -cs], 1), cat([cs, cc], 1)], 0)
    left = cat([rc, rs], 1)
    amap = aterm[0, my_b].astype(F32)
    amap = cat([amap, amap], 1)
    obs = observed[0, my_b, 0].astype(F32)
    live = iota((1, slots), 1) < counts[my_f, my_b, my_t]
    all_wt = weights[0, 0].astype(F32)
    own_wt = jnp.where(my_b == 0, all_wt[0:1, :], all_wt[1:2, :])
    wt = jnp.where(live, own_wt, 0.0)

    def take1(k, carry):
        peer, _, _ = peer_of(k)
        pltpu.make_async_copy(got1.at[peer], got1.at[peer], recv1.at[peer]).wait()
        return carry

    lax.fori_loop(1, n, take1, 0)
    sp = got1[...].astype(F32).reshape(n * rdev, 2 * M)
    sr = sp[:, :M]
    si = sp[:, M:]
    turned = cat([sr * ec - si * es, sr * es + si * ec], 1).astype(BF)
    t = mm(turned, kk[...]).astype(BF)
    tr = t[:, :size]
    ti = t[:, size:]
    image = mm(a_mat, cat([t, cat([-ti, tr], 1)], 0))
    weighted = (amap * image).astype(BF)
    z = mm(weighted, col_w)
    zr = z[:, :slots]
    zi = z[:, slots:]
    rcf = rc.astype(F32)
    rsf = rs.astype(F32)
    pred_re = jnp.sum(rcf * zr + rsf * zi, 0, keepdims=True) * (1.0 / size)
    pred_im = jnp.sum(rcf * zi - rsf * zr, 0, keepdims=True) * (1.0 / size)
    res_re = wt * (obs[0:1, :] - pred_re)
    res_im = wt * (obs[1:2, :] - pred_im)
    ccf = cc.astype(F32)
    csf = cs.astype(F32)
    s_re = (res_re * ccf - res_im * csf).astype(BF)
    s_im = (res_re * csf + res_im * ccf).astype(BF)
    grid = mm_nt(left, cat([cat([s_re, -s_im], 1), cat([s_im, s_re], 1)], 0))
    v = (amap * grid).astype(BF)
    u = mm(v, kb[...]).astype(BF)
    ur = u[:, :M]
    ui = u[:, M:]
    part = mm(ah, cat([u, cat([-ui, ur], 1)], 0))
    fold_out[...] = part.reshape(n, rdev, 2 * M).astype(BF)

    def copy2(k):
        peer, pf, pt = peer_of(k)
        return pltpu.make_async_remote_copy(
            src_ref=fold_out.at[peer],
            dst_ref=got2.at[me],
            send_sem=send2.at[k],
            recv_sem=recv2.at[me],
            device_id={"facet": pf, "team": pt, "sub": my_b},
            device_id_type=MESH,
        )

    def start2(k, carry):
        copy2(k).start()
        return carry

    lax.fori_loop(1, n, start2, 0)
    got2[me] = fold_out[me]

    def take2(k, carry):
        peer, _, _ = peer_of(k)
        pltpu.make_async_copy(got2.at[peer], got2.at[peer], recv2.at[peer]).wait()
        return carry

    lax.fori_loop(1, n, take2, 0)
    parts = got2[...].astype(F32).reshape(nf, nt, rdev, 2 * M)
    folded = jnp.sum(parts, 1)
    fr = folded[:, :, :M]
    fi = folded[:, :, M:]
    oc = own_c[None]
    os_ = own_s[None]
    fold3[...] = cat([fr * oc + fi * os_, fi * oc - fr * os_], 2).astype(BF)
    copy3 = pltpu.make_async_remote_copy(
        src_ref=fold3,
        dst_ref=got3,
        send_sem=send3,
        recv_sem=recv3,
        device_id={"facet": my_f, "team": my_t, "sub": other},
        device_id_type=MESH,
    )
    copy3.start()
    half = length // nb
    base = pl.multiple_of(my_b * half, 128)
    back = table[pl.ds(base, half), :]

    def update(stack, first):
        stack = stack.astype(F32).reshape(nf * rdev, 2 * M)
        turned = cat([stack[:, M:], -stack[:, :M]], 1)
        pre = mm_nt(cat([stack, turned], 0).astype(BF), back)
        tot_re = tot_im = None
        for a in range(nf):
            c = phi_c[first + a : first + a + 1, pl.ds(base, half)]
            s = phi_s[first + a : first + a + 1, pl.ds(base, half)]
            pr = pre[a * rdev : (a + 1) * rdev]
            pi = pre[h + a * rdev : h + (a + 1) * rdev]
            add_re = pr * c - pi * s
            add_im = pi * c + pr * s
            tot_re = add_re if tot_re is None else tot_re + add_re
            tot_im = add_im if tot_im is None else tot_im + add_im
        return tot_re, tot_im

    own_re, own_im = update(fold3[...], 0)
    copy3.wait_recv()
    oth_re, oth_im = update(got3[...], nf)
    out[0, 0] = own_re + oth_re
    out[0, 1] = own_im + oth_im

    def finish(k, carry):
        copy1(k).wait_send()
        copy2(k).wait_send()
        return carry

    lax.fori_loop(1, n, finish, 0)
    copy3.wait_send()


def tables(length, size):
    turn = np.arange(length)[:, None] * np.arange(M)[None, :] % length
    angle = turn * (TWO_PI / length)
    forward = np.concatenate([np.cos(angle), -np.sin(angle)], 1) / math.sqrt(length)
    angle = (np.arange(M)[:, None] * np.arange(size)[None, :] % size) * (TWO_PI / size)
    kc = np.cos(angle) / math.sqrt(M)
    ks = np.sin(angle) / math.sqrt(M)
    kk = np.block([[kc, ks], [-ks, kc]])
    kt = np.concatenate([kc.T, ks.T], 1)
    kb = np.block([[kc.T, -ks.T], [ks.T, kc.T]])
    return [np.asarray(v, np.float32).astype(ml_dtypes.bfloat16) for v in (forward, kk, kt, kb)]


def local(facet_rows, sub_offsets, facet_offsets, aterm, cells, observed, weights, counts):
    nf = lax.axis_size("facet")
    nt = lax.axis_size("team")
    nb = lax.axis_size("sub")
    rdev, length = facet_rows.shape[2:]
    size = aterm.shape[-1]
    n = nf * nt
    dims = (nf, nt, nb, length, size, rdev)
    consts = [jnp.asarray(v) for v in tables(length, size)]
    hbm = pl.BlockSpec(memory_space=pltpu.HBM)
    operands = [
        sub_offsets.T, facet_offsets.T, counts, facet_rows, aterm, cells, observed,
        weights.transpose(0, 2, 1, 3), *consts,
    ]
    dma = pltpu.SemaphoreType.DMA
    return pl.pallas_call(
        functools.partial(body, dims),
        out_shape=pltpu.VMEM((1, 2, rdev, length // nb), F32),
        in_specs=[hbm] * 12,
        out_specs=pl.BlockSpec(memory_space=pltpu.VMEM),
        scratch_shapes=[
            *[pltpu.SMEM(v.shape, v.dtype) for v in operands[:3]],
            *[pltpu.VMEM(v.shape, v.dtype) for v in operands[3:]],
            pltpu.VMEM((nb * nf, length), F32),
            pltpu.VMEM((nb * nf, length), F32),
            pltpu.VMEM((2 * nf, rdev, length), F32),
            pltpu.VMEM((nf, rdev, 2 * M), BF),
            pltpu.VMEM((n, rdev, 2 * M), BF),
            pltpu.VMEM((n, rdev, 2 * M), BF),
            pltpu.VMEM((n, rdev, 2 * M), BF),
            pltpu.VMEM((nf, rdev, 2 * M), BF),
            pltpu.VMEM((nf, rdev, 2 * M), BF),
            dma((n,)), dma((n,)), dma((n,)), dma((n,)), dma, dma, dma((12,)),
        ],
        compiler_params=pltpu.CompilerParams(
            collective_id=0, has_side_effects=True
        ),
    )(*operands)


def solution(mesh):
    placed = (
        P("facet", None, "team", None),
        P(),
        P(),
        P("facet", None, None, None),
        P("facet", None, "team", None, None),
        P("facet", None, "team", None, None),
        P("facet", None, "team", None),
        P(),
    )
    return jax.shard_map(
        local,
        mesh=mesh,
        in_specs=placed,
        out_specs=P("facet", None, "team", "sub"),
        check_vma=False,
    )
```

```python
import functools
import math

import jax
import jax.numpy as jnp
import ml_dtypes
import numpy as np
from jax import lax
from jax.experimental import pallas as pl
from jax.experimental.pallas import tpu as pltpu
from jax.sharding import PartitionSpec as P

M = 128
TWO_PI = 2.0 * math.pi
BF = jnp.bfloat16
F32 = jnp.float32
MESH = pl.DeviceIdType.MESH


def sincos(turns, period):
    shift = period.bit_length() - 3
    quad = (turns + (1 << (shift - 1))) >> shift
    t = (turns - (quad << shift)).astype(F32) * (TWO_PI / period)
    t2 = t * t
    s = t * (1.0 + t2 * (-1.0 / 6 + t2 * (1.0 / 120 + t2 * (-1.0 / 5040))))
    c = 1.0 + t2 * (-0.5 + t2 * (1.0 / 24 + t2 * (-1.0 / 720 + t2 * (1.0 / 40320))))
    odd = (quad & 1) != 0
    cos = jnp.where(odd, s, c)
    sin = jnp.where(odd, c, s)
    cos = jnp.where(((quad + 1) & 2) != 0, -cos, cos)
    sin = jnp.where((quad & 2) != 0, -sin, sin)
    return cos, sin


def mm(left, right):
    return jnp.dot(left, right, preferred_element_type=F32)


def mm_nt(left, right):
    return lax.dot_general(left, right, (((1,), (1,)), ((), ())), preferred_element_type=F32)


def cat(parts, axis):
    return jnp.concatenate(parts, axis)


def iota(shape, dim):
    return lax.broadcasted_iota(jnp.int32, shape, dim)


def body(
    dims,
    *refs,
):
    ins = refs[:12]
    out = refs[12]
    bufs = refs[13:25]
    (
    phi_c, phi_s, x_buf, spec_out, got1, fold_out, got2,
    send1, recv1, send2, recv2, in_sem,
    ) = refs[25:]
    sub_off, fac_off, counts, rows, aterm, cells, observed, weights, table, kk, kt, kb = bufs
    nf, nt, nb, length, size, rdev = dims
    rall = rdev * nt
    n = nf * nt
    slots = cells.shape[-1]
    period = 4 * size
    my_f = lax.axis_index("facet")
    my_t = lax.axis_index("team")
    my_b = lax.axis_index("sub")
    me = my_f * nt + my_t
    other = 1 - my_b

    def peer_of(k):
        peer = lax.rem(me + k, n)
        return peer, peer // nt, lax.rem(peer, nt)

    barrier = pltpu.get_barrier_semaphore()

    def greet(k, carry):
        _, pf, pt = peer_of(k)
        pl.semaphore_signal(
            barrier, inc=1, device_id={"facet": pf, "team": pt, "sub": my_b}, device_id_type=MESH
        )
        return carry

    lax.fori_loop(1, n, greet, 0)
    pl.semaphore_signal(
        barrier, inc=1, device_id={"facet": my_f, "team": my_t, "sub": other}, device_id_type=MESH
    )

    fetches = [pltpu.make_async_copy(ins[i], bufs[i], in_sem.at[i]) for i in range(12)]
    for i in (0, 3, 8, 1, 5, 10, 9, 4, 2, 6, 7, 11):
        fetches[i].start()
    fetches[0].wait()

    sub_row = iota((nb * nf, 1), 0)
    tune = jnp.zeros((nb * nf, 1), jnp.int32)
    for s in range(nf):
        tune = jnp.where(sub_row == s, sub_off[1, s * nb + my_b], tune)
        tune = jnp.where(sub_row == nf + s, sub_off[1, s * nb + other], tune)
    pc, ps = sincos(iota((nb * nf, length), 1) * tune, length)
    phi_c[...] = pc
    phi_s[...] = ps
    fetches[3].wait()
    re = rows[0, 0].astype(F32)
    im = rows[0, 1].astype(F32)
    for a in range(nf):
        c = phi_c[a : a + 1, :]
        s = phi_s[a : a + 1, :]
        x_buf[a] = re * c + im * s
        x_buf[nf + a] = im * c - re * s
    x = x_buf[...].reshape(2 * nf * rdev, length).astype(BF)
    fetches[8].wait()
    y = mm(x, table[...])
    h = nf * rdev
    spec = cat([y[:h, :M] - y[h:, M:], y[:h, M:] + y[h:, :M]], 1)
    spec_out[...] = spec.reshape(nf, rdev, 2 * M).astype(BF)

    pl.semaphore_wait(barrier, n)

    def copy1(k):
        peer, pf, pt = peer_of(k)
        return pltpu.make_async_remote_copy(
            src_ref=spec_out.at[pf],
            dst_ref=got1.at[me],
            send_sem=send1.at[k],
            recv_sem=recv1.at[me],
            device_id={"facet": pf, "team": pt, "sub": my_b},
            device_id_type=MESH,
        )

    def start1(k, carry):
        copy1(k).start()
        return carry

    lax.fori_loop(1, n, start1, 0)
    got1[me] = spec_out[my_f]

    for i in (1, 5, 10, 9, 4, 2, 6, 7, 11):
        fetches[i].wait()
    shift_u = sub_off[0, my_f * nb + my_b]
    step = length // rall
    scale_g = 1.0 / math.sqrt(rall * nf)
    lane = iota((1, n * rdev), 1)
    col_a = jnp.zeros((1, n * rdev), jnp.int32)
    row = iota((n * rdev, 1), 0)
    row_a = jnp.zeros((n * rdev, 1), jnp.int32)
    row_c = jnp.zeros((n * rdev, 1), jnp.int32)
    for f in range(nf):
        col_a = jnp.where(lane // rall == f, fac_off[0, f], col_a)
        row_a = jnp.where(row // rall == f, fac_off[0, f], row_a)
        row_c = jnp.where(row // rall == f, fac_off[1, f], row_c)
    p0 = iota((M, n * rdev), 0)
    gc, gs = sincos(p0 * col_a - (p0 + shift_u) * (lane % rall * step), length)
    gc = (gc * scale_g).astype(BF)
    gs = (gs * scale_g).astype(BF)
    a_mat = mm(kt[...], cat([cat([gc, gs], 1), cat([-gs, gc], 1)], 0)).astype(BF)
    p1 = iota((n * rdev, M), 1)
    hc, hs = sincos(p1 * row_a - (p1 + shift_u) * (row % rall * step), length)
    at = mm(cat([hc * scale_g, hs * scale_g], 1).astype(BF), kk[...])
    ah = cat([at[:, :size], -at[:, size:]], 1).astype(BF)
    ec, es = sincos(p1 * row_c, length)
    own_scale = math.sqrt(length / M) / size
    own_c, own_s = sincos(iota((rdev, M), 1) * fac_off[1, my_f], length)
    own_c = own_c * own_scale
    own_s = own_s * own_scale
    pair = cells[0, my_b, 0]
    index = iota((size, slots), 0)
    rc, rs = sincos(index * pair[0:1, :], period)
    rc = rc.astype(BF)
    rs = rs.astype(BF)
    cc, cs = sincos(index * pair[1:2, :], period)
    cc = cc.astype(BF)
    cs = cs.astype(BF)
    col_w = cat([cat([cc, -cs], 1), cat([cs, cc], 1)], 0)
    left = cat([rc, rs], 1)
    amap = aterm[0, my_b].astype(F32)
    amap = cat([amap, amap], 1)
    obs = observed[0, my_b, 0].astype(F32)
    live = iota((1, slots), 1) < counts[my_f, my_b, my_t]
    all_wt = weights[0, 0].astype(F32)
    own_wt = jnp.where(my_b == 0, all_wt[0:1, :], all_wt[1:2, :])
    wt = jnp.where(live, own_wt, 0.0)

    def take1(k, carry):
        peer, _, _ = peer_of(k)
        pltpu.make_async_copy(got1.at[peer], got1.at[peer], recv1.at[peer]).wait()
        return carry

    lax.fori_loop(1, n, take1, 0)
    sp = got1[...].astype(F32).reshape(n * rdev, 2 * M)
    sr = sp[:, :M]
    si = sp[:, M:]
    turned = cat([sr * ec - si * es, sr * es + si * ec], 1).astype(BF)
    t = mm(turned, kk[...]).astype(BF)
    tr = t[:, :size]
    ti = t[:, size:]
    image = mm(a_mat, cat([t, cat([-ti, tr], 1)], 0))
    weighted = (amap * image).astype(BF)
    z = mm(weighted, col_w)
    zr = z[:, :slots]
    zi = z[:, slots:]
    rcf = rc.astype(F32)
    rsf = rs.astype(F32)
    pred_re = jnp.sum(rcf * zr + rsf * zi, 0, keepdims=True) * (1.0 / size)
    pred_im = jnp.sum(rcf * zi - rsf * zr, 0, keepdims=True) * (1.0 / size)
    res_re = wt * (obs[0:1, :] - pred_re)
    res_im = wt * (obs[1:2, :] - pred_im)
    ccf = cc.astype(F32)
    csf = cs.astype(F32)
    s_re = (res_re * ccf - res_im * csf).astype(BF)
    s_im = (res_re * csf + res_im * ccf).astype(BF)
    grid = mm_nt(left, cat([cat([s_re, -s_im], 1), cat([s_im, s_re], 1)], 0))
    v = (amap * grid).astype(BF)
    u = mm(v, kb[...]).astype(BF)
    ur = u[:, :M]
    ui = u[:, M:]
    part = mm(ah, cat([u, cat([-ui, ur], 1)], 0))
    fold_out[...] = part.reshape(n, rdev, 2 * M).astype(BF)

    def copy2(k, far):
        peer, pf, pt = peer_of(k)
        return pltpu.make_async_remote_copy(
            src_ref=fold_out.at[peer],
            dst_ref=got2.at[far, me],
            send_sem=send2.at[far, k],
            recv_sem=recv2.at[far, me],
            device_id={"facet": pf, "team": pt, "sub": other if far else my_b},
            device_id_type=MESH,
        )

    def start2(k, carry):
        copy2(k, 1).start()
        copy2(k, 0).start()
        return carry

    copy2(0, 1).start()
    lax.fori_loop(1, n, start2, 0)
    got2[0, me] = fold_out[me]

    def take2(far):
        def step(k, carry):
            peer, _, _ = peer_of(k)
            slot = got2.at[far, peer]
            pltpu.make_async_copy(slot, slot, recv2.at[far, peer]).wait()
            return carry

        lax.fori_loop(1 - far, n, step, 0)
        parts = got2[far].astype(F32).reshape(nf, nt, rdev, 2 * M)
        folded = jnp.sum(parts, 1)
        fr = folded[:, :, :M]
        fi = folded[:, :, M:]
        oc = own_c[None]
        os_ = own_s[None]
        return cat([fr * oc + fi * os_, fi * oc - fr * os_], 2)

    half = length // nb
    base = pl.multiple_of(my_b * half, 128)
    back = table[pl.ds(base, half), :]

    def update(stack, first):
        stack = stack.reshape(nf * rdev, 2 * M)
        turned = cat([stack[:, M:], -stack[:, :M]], 1)
        pre = mm_nt(cat([stack, turned], 0).astype(BF), back)
        tot_re = tot_im = None
        for a in range(nf):
            c = phi_c[first + a : first + a + 1, pl.ds(base, half)]
            s = phi_s[first + a : first + a + 1, pl.ds(base, half)]
            pr = pre[a * rdev : (a + 1) * rdev]
            pi = pre[h + a * rdev : h + (a + 1) * rdev]
            add_re = pr * c - pi * s
            add_im = pi * c + pr * s
            tot_re = add_re if tot_re is None else tot_re + add_re
            tot_im = add_im if tot_im is None else tot_im + add_im
        return tot_re, tot_im

    own_re, own_im = update(take2(0), 0)
    oth_re, oth_im = update(take2(1), nf)
    out[0, 0] = own_re + oth_re
    out[0, 1] = own_im + oth_im

    def finish(k, carry):
        copy1(k).wait_send()
        copy2(k, 0).wait_send()
        copy2(k, 1).wait_send()
        return carry

    lax.fori_loop(1, n, finish, 0)
    copy2(0, 1).wait_send()


def tables(length, size):
    turn = np.arange(length)[:, None] * np.arange(M)[None, :] % length
    angle = turn * (TWO_PI / length)
    forward = np.concatenate([np.cos(angle), -np.sin(angle)], 1) / math.sqrt(length)
    angle = (np.arange(M)[:, None] * np.arange(size)[None, :] % size) * (TWO_PI / size)
    kc = np.cos(angle) / math.sqrt(M)
    ks = np.sin(angle) / math.sqrt(M)
    kk = np.block([[kc, ks], [-ks, kc]])
    kt = np.concatenate([kc.T, ks.T], 1)
    kb = np.block([[kc.T, -ks.T], [ks.T, kc.T]])
    return [np.asarray(v, np.float32).astype(ml_dtypes.bfloat16) for v in (forward, kk, kt, kb)]


def local(facet_rows, sub_offsets, facet_offsets, aterm, cells, observed, weights, counts):
    nf = lax.axis_size("facet")
    nt = lax.axis_size("team")
    nb = lax.axis_size("sub")
    rdev, length = facet_rows.shape[2:]
    size = aterm.shape[-1]
    n = nf * nt
    dims = (nf, nt, nb, length, size, rdev)
    consts = [jnp.asarray(v) for v in tables(length, size)]
    hbm = pl.BlockSpec(memory_space=pltpu.HBM)
    operands = [
        sub_offsets.T, facet_offsets.T, counts, facet_rows, aterm, cells, observed,
        weights.transpose(0, 2, 1, 3), *consts,
    ]
    dma = pltpu.SemaphoreType.DMA
    return pl.pallas_call(
        functools.partial(body, dims),
        out_shape=pltpu.VMEM((1, 2, rdev, length // nb), F32),
        in_specs=[hbm] * 12,
        out_specs=pl.BlockSpec(memory_space=pltpu.VMEM),
        scratch_shapes=[
            *[pltpu.SMEM(v.shape, v.dtype) for v in operands[:3]],
            *[pltpu.VMEM(v.shape, v.dtype) for v in operands[3:]],
            pltpu.VMEM((nb * nf, length), F32),
            pltpu.VMEM((nb * nf, length), F32),
            pltpu.VMEM((2 * nf, rdev, length), F32),
            pltpu.VMEM((nf, rdev, 2 * M), BF),
            pltpu.VMEM((n, rdev, 2 * M), BF),
            pltpu.VMEM((n, rdev, 2 * M), BF),
            pltpu.VMEM((nb, n, rdev, 2 * M), BF),
            dma((n,)), dma((n,)), dma((nb, n)), dma((nb, n)), dma((12,)),
        ],
        compiler_params=pltpu.CompilerParams(
            collective_id=0, has_side_effects=True
        ),
    )(*operands)


def solution(mesh):
    placed = (
        P("facet", None, "team", None),
        P(),
        P(),
        P("facet", None, None, None),
        P("facet", None, "team", None, None),
        P("facet", None, "team", None, None),
        P("facet", None, "team", None),
        P(),
    )
    return jax.shard_map(
        local,
        mesh=mesh,
        in_specs=placed,
        out_specs=P("facet", None, "team", "sub"),
        check_vma=False,
    )
```
